32 devices in a mesh: year: 8 (over y, x, core), port: 4 (over z).
Axes of the slice: x: 2, y: 2, z: 4, core: 2. Of those that a mesh axis runs over, the one named last changes fastest.
Arguments:
- event_loss: bfloat16 [4096, 4096], P('year', 'port'), may hold values from 0 to 24
- event_year: int32 [4096], P('year'), may hold values from -1 to 255, as said below
- retention: float32 [4096], P('port'), may hold values from 0.2 to 2
- risk_limit: float32 [4096], P('port'), may hold values from 1 to 8
- cession_share: bfloat16 [4096, 4], P('port'), may hold values from 0.099609375 to 1
- member_treaty: int32 [4096, 4], P('port'), may hold values from 0 to 1023, all different within a row
- attach_tier: int32 [1024], P('port'), may hold values from 2 to 11
- limit_tier: int32 [1024], P('port'), may hold values from 2 to 10
- reinstatements: int32 [1024], P('port'), may hold values from 0 to 3
- reinstate_rate: float32 [1024], P('port'), may hold values from 0.1 to 1
- stop_attach: float32 [1024], P('port'), may hold values from 0.7 to 2
- stop_width: float32 [1024], P('port'), may hold values from 0.3 to 2
Outputs:
- layer_net: float32 [1024, 256], P('port', 'year')
- stop_loss: float32 [1024, 256], P('port', 'year')
- tail_mean: float32 [1024], P('port')
The draws below stay inside these ranges and needn't reach their ends.
Inputs may be any that keep to these rules, and one draw needn't show every extreme that they name: `event_year`: the 512 rows of year-block b name years b * 32 to (b + 1) * 32 - 1 in nondecreasing order, followed by padding rows marked -1; at least one block has no padding row. `member_treaty`: each portfolio names 4 different treaties, and every treaty is named by some portfolio.
All inputs are finite; a program needn't handle non-finite values.
Results may differ from the reference program's by a relative error of at most 0.029.
Values may be sent and summed in bfloat16 or wider, within the bound.
A program may use at most 64 MiB of HBM per device.

```python
import math
import jax
import jax.numpy as jnp
from jax import lax

PORT_DEV = 1024
TREATIES = 1024
MEMB = 4
YEAR_DEV = 32
TAIL = 16
ROWS_DEV = 512
PORTS = 4096
YEARS = 256
EVENT_ROWS = 4096
N_YEAR = 8
N_PORT = 4


def draw_event_loss(key, part):
    key_row, key_col, key_cell = jax.random.split(key, 3)
    position = jnp.arange(EVENT_ROWS, dtype=jnp.float32) / EVENT_ROWS
    rising = jnp.exp(math.log(3.0) * position)
    col_scale = jnp.exp(jax.random.uniform(key_col, (PORTS,), jnp.float32, math.log(0.3), math.log(3.0)))
    row_scale = jnp.exp(jax.random.uniform(key_row, (EVENT_ROWS,), jnp.float32, math.log(0.5), math.log(2.0)))
    cell = jnp.exp(jax.random.uniform(key_cell, (EVENT_ROWS, PORTS), jnp.float32, math.log(0.2), math.log(5.0)))
    value = 0.2 * (rising * row_scale)[:, None] * col_scale[None, :] * cell
    return value.astype(jnp.bfloat16)


def draw_event_year(key, part):
    key_fill, key_full, key_year = jax.random.split(key, 3)
    block_total = EVENT_ROWS // ROWS_DEV
    halvings = jax.random.randint(key_fill, (block_total,), 0, 4).astype(jnp.int32)
    live_rows = jnp.right_shift(jnp.full((block_total,), ROWS_DEV, jnp.int32), halvings)
    full_block = jax.random.randint(key_full, (), 0, block_total).astype(jnp.int32)
    block_index = jnp.arange(block_total, dtype=jnp.int32)
    live_rows = jnp.where(block_index == full_block, ROWS_DEV, live_rows)
    years = jax.random.randint(key_year, (block_total, ROWS_DEV), 0, YEAR_DEV).astype(jnp.int32)
    slot_index = jnp.arange(ROWS_DEV, dtype=jnp.int32)
    years = jnp.where(slot_index[None, :] < live_rows[:, None], years, YEAR_DEV)
    years = jnp.sort(years, axis=1)
    marked = jnp.where(years < YEAR_DEV, years + block_index[:, None] * YEAR_DEV, -1)
    return marked.reshape(EVENT_ROWS).astype(jnp.int32)


def set_ends(entries, rng, smallest, high):
    place = [jax.random.randint(jax.random.fold_in(rng, axis), (), 0, length) for axis, length in enumerate(entries.shape)]
    main_axis = entries.shape.index(max(entries.shape))
    next_to = place[:main_axis] + [(place[main_axis] + 1) % entries.shape[main_axis]] + place[main_axis + 1:]
    return entries.at[tuple(place)].set(smallest).at[tuple(next_to)].set(high)


def block_levels(key, dims, pieces, smallest, top_value):
    def one(dim, parts):
        draws = jax.random.uniform(jax.random.fold_in(jax.random.fold_in(key, 6), dim), (parts,), jnp.float32, smallest / len(pieces), top_value / len(pieces))
        return jnp.repeat(jnp.exp(draws), dims[dim] // parts).reshape((-1,) + (1,) * (len(dims) - dim - 1))

    level = one(*pieces[0])
    for cut in pieces[1:]:
        level = level * one(*cut)
    return level


def distinct(stream_key, rows, count, top, lift):
    sequence = jax.random.permutation(jax.random.fold_in(stream_key, 1), count)
    boost = sequence
    for power in range(3):
        boost = boost * boost // count
    boost = boost * lift // count
    lots = jax.random.randint(jax.random.fold_in(stream_key, 2), (rows, count), 0, 4096) + boost
    sure = jax.random.permutation(jax.random.fold_in(stream_key, 3), rows)[jnp.arange(count) % rows]
    lots = jnp.where(jnp.arange(rows)[:, None] == sure[None, :], 1 << 14, lots)
    merit = lots * count + jnp.arange(count)
    return lax.top_k(merit.astype(jnp.int32), top)[1].astype(jnp.int32)


def setup_inputs(seed: int = 0) -> dict:
    streams_of = jax.random.split(jax.random.key(seed), 13)
    return {
        "event_loss": draw_event_loss(jax.random.fold_in(streams_of[12], 71), 0),
        "event_year": draw_event_year(jax.random.fold_in(streams_of[12], 71), 0),
        "retention": jnp.clip(jnp.exp(math.log(2.0) - 2.3025851 * jax.random.uniform(streams_of[2], (PORTS,), jnp.float32) ** block_levels(streams_of[2], (PORTS,), ((0, 4),), -0.2, 0.2)), 0.2, 2.0),
        "risk_limit": jnp.clip(jnp.exp(math.log(8.0) - 2.0794415 * jax.random.uniform(streams_of[3], (PORTS,), jnp.float32) ** block_levels(streams_of[3], (PORTS,), ((0, 4),), -0.2, 0.2)), 1.0, 8.0),
        "cession_share": jnp.clip(jnp.exp(math.log(1.0) - 2.306499 * jax.random.uniform(streams_of[4], (PORTS, MEMB), jnp.float32) ** block_levels(streams_of[4], (PORTS, MEMB), ((0, 4),), -0.2, 0.2)), 0.099609375, 1.0).astype(jnp.bfloat16),
        "member_treaty": distinct(streams_of[5], PORTS, TREATIES, MEMB, 32),
        "attach_tier": set_ends(jax.random.randint(streams_of[6], (TREATIES,), 2, 12), jax.random.fold_in(streams_of[6], 1), 2, 11).astype(jnp.int32),
        "limit_tier": set_ends(jax.random.randint(streams_of[7], (TREATIES,), 2, 11), jax.random.fold_in(streams_of[7], 1), 2, 10).astype(jnp.int32),
        "reinstatements": set_ends(jax.random.randint(streams_of[8], (TREATIES,), 0, 4), jax.random.fold_in(streams_of[8], 1), 0, 3).astype(jnp.int32),
        "reinstate_rate": jnp.clip(jnp.exp(math.log(1.0) - 2.3025851 * jax.random.uniform(streams_of[9], (TREATIES,), jnp.float32) ** block_levels(streams_of[9], (TREATIES,), ((0, 4),), -0.2, 0.2)), 0.1, 1.0),
        "stop_attach": jnp.clip(jnp.exp(math.log(2.0) - 1.0498221 * jax.random.uniform(streams_of[10], (TREATIES,), jnp.float32) ** block_levels(streams_of[10], (TREATIES,), ((0, 4),), -0.2, 0.2)), 0.7, 2.0),
        "stop_width": jnp.clip(jnp.exp(math.log(2.0) - 1.89712 * jax.random.uniform(streams_of[11], (TREATIES,), jnp.float32) ** block_levels(streams_of[11], (TREATIES,), ((0, 4),), -0.2, 0.2)), 0.3, 2.0),
    }


UNIT_LOSS = 1.0


def clamp_between(values, lower, upper):
    return jnp.minimum(jnp.maximum(values, lower), upper)


def block_tables(loss_block, year_block, first_year, retention, risk_limit, cession_share, member_treaty, attach_tier, limit_tier):
    ceded_loss = clamp_between(loss_block.astype(jnp.float32) - retention[None, :], 0.0, risk_limit[None, :]).astype(jnp.bfloat16)
    ceded_cols = lax.optimization_barrier(ceded_loss).astype(jnp.float32).T
    shard_ids = (jnp.arange(PORT_DEV * N_PORT, dtype=jnp.int32) // PORT_DEV) * TREATIES
    shard_sums = jnp.zeros((N_PORT * TREATIES, ceded_cols.shape[1]), jnp.float32)
    for member_slot in range(MEMB):
        weight_col = cession_share[:, member_slot].astype(jnp.float32)
        segment_ids = (shard_ids + member_treaty[:, member_slot]).astype(jnp.int32)
        shard_sums = shard_sums + jax.ops.segment_sum(ceded_cols * weight_col[:, None], segment_ids, N_PORT * TREATIES)
    rounded = lax.optimization_barrier(shard_sums.astype(jnp.bfloat16)).astype(jnp.float32)
    event_treaty = jnp.sum(rounded.reshape(N_PORT, TREATIES, ceded_cols.shape[1]), axis=0)
    attach = attach_tier.astype(jnp.float32) * UNIT_LOSS
    limit_loss = limit_tier.astype(jnp.float32) * UNIT_LOSS
    recovered = clamp_between(event_treaty - attach[:, None], 0.0, limit_loss[:, None])
    retained = event_treaty - recovered
    local_year = (year_block - first_year).astype(jnp.int32)
    year_hits = (local_year[:, None] == jnp.arange(YEAR_DEV, dtype=jnp.int32)[None, :]).astype(jnp.float32)
    annual = jnp.dot(recovered, year_hits, precision=lax.Precision.HIGHEST, preferred_element_type=jnp.float32)
    kept_annual = jnp.dot(retained, year_hits, precision=lax.Precision.HIGHEST, preferred_element_type=jnp.float32)
    return annual, kept_annual


def reference(event_loss, event_year, retention, risk_limit, cession_share, member_treaty, attach_tier, limit_tier, reinstatements, reinstate_rate, stop_attach, stop_width):
    loss_blocks = event_loss.reshape(N_YEAR, ROWS_DEV, PORTS)
    year_blocks = event_year.reshape(N_YEAR, ROWS_DEV)
    first_years = jnp.arange(N_YEAR, dtype=jnp.int32) * YEAR_DEV

    def one_block(inputs):
        return block_tables(inputs[0], inputs[1], inputs[2], retention, risk_limit, cession_share, member_treaty, attach_tier, limit_tier)

    annual, kept_annual = lax.map(one_block, (loss_blocks, year_blocks, first_years))
    annual = jnp.transpose(annual, (1, 0, 2)).reshape(TREATIES, YEARS)
    kept_annual = jnp.transpose(kept_annual, (1, 0, 2)).reshape(TREATIES, YEARS)
    limit_loss = limit_tier.astype(jnp.float32) * UNIT_LOSS
    reinstated = reinstatements.astype(jnp.float32)
    layer_paid = jnp.minimum(annual, ((1.0 + reinstated) * limit_loss)[:, None])
    layer_net = (layer_paid - reinstate_rate[:, None] * jnp.minimum(layer_paid, (reinstated * limit_loss)[:, None])) / limit_loss[:, None]
    base_loss = UNIT_LOSS + jnp.sum(kept_annual, axis=1) / YEARS
    loss_ratio = kept_annual / base_loss[:, None]
    stop_loss = clamp_between(loss_ratio - stop_attach[:, None], 0.0, stop_width[:, None])
    tail_mean = jnp.mean(jnp.sort(loss_ratio, axis=1)[:, YEARS - TAIL:], axis=1)
    return layer_net, stop_loss, tail_mean
```

```python
import functools

import jax
import jax.numpy as jnp
from jax import lax
from jax.experimental import pallas as pl
from jax.experimental.pallas import tpu as pltpu
from jax.sharding import PartitionSpec as P

TREATIES = 1024
YEAR_DEV = 32
TAIL = 16
LANES = 128
SUBLANES = 8
UNIT_LOSS = 1.0
MESH = pl.DeviceIdType.MESH


def clamp_between(values, lower, upper):
    return jnp.minimum(jnp.maximum(values, lower), upper)


def exchange(items, low, high):
    larger = jnp.maximum(items[low], items[high])
    items[high] = jnp.minimum(items[low], items[high])
    items[low] = larger


def sort_network(count):
    pairs = []
    width = 1
    while width < count:
        step = width
        while step >= 1:
            for start in range(step % width, count - step, 2 * step):
                for offset in range(min(step, count - start - step)):
                    low = start + offset
                    if low // (2 * width) == (low + step) // (2 * width):
                        pairs.append((low, low + step))
            step //= 2
        width *= 2
    return pairs


def sort_falling(items):
    items = list(items)
    for low, high in sort_network(len(items)):
        exchange(items, low, high)
    return items


def merge_largest(first, second, ordered):
    count = len(first)
    items = [jnp.maximum(first[i], second[count - 1 - i]) for i in range(count)]
    step = count // 2
    while ordered and step >= 1:
        for low in range(count):
            if low & step == 0:
                exchange(items, low, low + step)
        step //= 2
    return items


def largest_sum(values):
    rows = values.shape[0]
    tiles = [values[start : start + SUBLANES] for start in range(0, rows, SUBLANES)]
    runs = [sort_falling(tiles[start : start + TAIL]) for start in range(0, len(tiles), TAIL)]
    while len(runs) > 1:
        merged = [
            merge_largest(runs[i], runs[i + 1], True) for i in range(0, len(runs) - 1, 2)
        ]
        runs = merged + runs[len(merged) * 2 :]
    best = runs[0]
    shift = SUBLANES // 2
    while shift >= 1:
        rolled = [pltpu.roll(item, shift, 0) for item in best]
        best = merge_largest(best, rolled, shift > 1)
        shift //= 2
    total = best[0]
    for item in best[1:]:
        total = total + item
    return total[0:1]


def kernel(
    sizes,
    loss_ref,
    year_ref,
    retention_ref,
    risk_ref,
    share_ref,
    member_ref,
    attach_ref,
    limit_ref,
    reinst_ref,
    rate_ref,
    stop_attach_ref,
    stop_width_ref,
    net_ref,
    stop_ref,
    tail_ref,
    ceded,
    sending,
    landing,
    held,
    own_sum,
    kept,
    port_send,
    port_recv,
    year_send,
    year_recv,
):
    n_year, n_port, own, groups = sizes
    rows, ports = loss_ref.shape
    me_port = lax.axis_index("port")
    me_year = lax.axis_index("year")

    barrier = pltpu.get_barrier_semaphore()
    for step in range(1, n_port):
        peer = lax.rem(me_port + step, n_port)
        pl.semaphore_signal(barrier, inc=1, device_id={"port": peer}, device_id_type=MESH)
    for step in range(1, n_year):
        peer = lax.rem(me_year + step, n_year)
        pl.semaphore_signal(barrier, inc=1, device_id={"year": peer}, device_id_type=MESH)

    ceded[...] = clamp_between(
        loss_ref[...].astype(jnp.float32) - retention_ref[...], 0.0, risk_ref[...]
    ).astype(jnp.bfloat16)

    def product(dest, group):
        lane = lax.broadcasted_iota(jnp.int32, (LANES, ports), 0) + group * LANES
        treaty = lane + dest * own
        if own % LANES:
            treaty = jnp.where(lane < own, treaty, -1)
        weights = jnp.zeros((LANES, ports), jnp.float32)
        for slot in range(member_ref.shape[0]):
            weights = jnp.where(
                member_ref[slot : slot + 1, :] == treaty,
                share_ref[slot : slot + 1, :].astype(jnp.float32),
                weights,
            )
        return lax.dot_general(
            ceded[...],
            weights.astype(jnp.bfloat16),
            (((1,), (1,)), ((), ())),
            preferred_element_type=jnp.float32,
        )

    def port_copy(piece, group, device, slot):
        return pltpu.make_async_remote_copy(
            src_ref=sending.at[piece, group],
            dst_ref=landing.at[slot, group],
            send_sem=port_send.at[piece, group],
            recv_sem=port_recv.at[slot, group],
            device_id={"port": device},
            device_id_type=MESH,
        )

    def wait_landed(slot, group):
        port_copy(0, group, me_port, slot).wait_recv()

    waited = []

    def entered():
        if not waited:
            pl.semaphore_wait(barrier, n_port + n_year - 2)
            waited.append(True)

    copies = []
    if n_port == 4:
        is_end = (me_port == 0) | (me_port == 3)
        near = me_port + 1 - 2 * lax.rem(me_port, 2)
        low_half = me_port < 2
        far_end = jnp.where(low_half, 3, 0)
        far_middle = jnp.where(low_half, 2, 1)
        for group in range(groups):
            dest = jnp.where(is_end, far_middle, far_end)
            sending[0, group] = product(dest, group).astype(jnp.bfloat16)
            entered()
            copy = port_copy(0, group, jnp.where(is_end, near, far_end), 2)
            copy.start()
            copies.append(copy)

            dest = jnp.where(is_end, far_end, near)
            sending[1, group] = product(dest, group).astype(jnp.bfloat16)
            copy = port_copy(1, group, dest, jnp.where(is_end, 1, 0))
            copy.start()
            copies.append(copy)

            last = product(jnp.where(is_end, near, far_middle), group)
            held[group] = last
            copy = port_copy(
                2, group, jnp.where(is_end, near, far_middle), jnp.where(is_end, 0, 1)
            )
            copies.append(copy)

            @pl.when(is_end)
            def _():
                sending[2, group] = held[group].astype(jnp.bfloat16)
                copy.start()

        for group in range(groups):
            own_sum[group] = product(me_port, group)
        for group in range(groups):
            copy = copies[3 * group + 2]

            @pl.when(jnp.logical_not(is_end))
            def _():
                wait_landed(2, group)
                sending[2, group] = (
                    held[group] + landing[2, group].astype(jnp.float32)
                ).astype(jnp.bfloat16)
                copy.start()

    else:
        for group in range(groups):
            for step in range(1, n_port):
                dest = lax.rem(me_port + step, n_port)
                sending[step - 1, group] = product(dest, group).astype(jnp.bfloat16)
                entered()
                copy = port_copy(step - 1, group, dest, step - 1)
                copy.start()
                copies.append(copy)
        for group in range(groups):
            own_sum[group] = product(me_port, group)
    entered()

    local_year = year_ref[...] - me_year * YEAR_DEV
    hits = (
        (local_year == lax.broadcasted_iota(jnp.int32, (YEAR_DEV, rows), 0))
        .astype(jnp.float32)
        .astype(jnp.bfloat16)
    )

    def split_dot(values):
        upper = values.astype(jnp.bfloat16)
        lower = (values - upper.astype(jnp.float32)).astype(jnp.bfloat16)
        return jnp.dot(hits, upper, preferred_element_type=jnp.float32) + jnp.dot(
            hits, lower, preferred_element_type=jnp.float32
        )

    def year_copy(step, group):
        return pltpu.make_async_remote_copy(
            src_ref=kept.at[group, me_year],
            dst_ref=kept.at[group, me_year],
            send_sem=year_send.at[group, step - 1],
            recv_sem=year_recv.at[group, me_year],
            device_id={"year": lax.rem(me_year + step, n_year)},
            device_id_type=MESH,
        )

    for group in range(groups):
        lanes = slice(group * LANES, (group + 1) * LANES)
        event_treaty = own_sum[group]
        if n_port == 4:
            wait_landed(0, group)
            wait_landed(1, group)

            @pl.when(is_end)
            def _():
                wait_landed(2, group)

            event_treaty = event_treaty + landing[0, group].astype(jnp.float32)
            event_treaty = event_treaty + landing[1, group].astype(jnp.float32)
            event_treaty = event_treaty + jnp.where(
                is_end, landing[2, group].astype(jnp.float32), 0.0
            )
        else:
            for slot in range(n_port - 1):
                wait_landed(slot, group)
                event_treaty = event_treaty + landing[slot, group].astype(jnp.float32)
        attach = attach_ref[:, lanes].astype(jnp.float32) * UNIT_LOSS
        limit_loss = limit_ref[:, lanes].astype(jnp.float32) * UNIT_LOSS
        recovered = clamp_between(event_treaty - attach, 0.0, limit_loss)
        retained = event_treaty - recovered
        yearly = split_dot(jnp.concatenate((recovered, retained), 1))
        annual = yearly[:, :LANES]
        kept[group, me_year] = yearly[:, LANES:]
        for step in range(1, n_year):
            copy = year_copy(step, group)
            copy.start()
            copies.append(copy)
        reinstated = reinst_ref[:, lanes].astype(jnp.float32)
        layer_paid = jnp.minimum(annual, (1.0 + reinstated) * limit_loss)
        net_ref[:, lanes] = (
            layer_paid
            - rate_ref[:, lanes] * jnp.minimum(layer_paid, reinstated * limit_loss)
        ) / limit_loss

    for group in range(groups):
        lanes = slice(group * LANES, (group + 1) * LANES)
        for step in range(1, n_year):
            source = lax.rem(me_year + step, n_year)
            pltpu.make_async_remote_copy(
                src_ref=kept.at[group, source],
                dst_ref=kept.at[group, source],
                send_sem=year_send.at[group, step - 1],
                recv_sem=year_recv.at[group, source],
                device_id={"year": source},
                device_id_type=MESH,
            ).wait_recv()
        every = kept[group].reshape(n_year * YEAR_DEV, LANES)
        base_loss = UNIT_LOSS + jnp.sum(every, axis=0, keepdims=True) / (n_year * YEAR_DEV)
        tail_ref[:, lanes] = largest_sum(every) / base_loss / TAIL
        loss_ratio = kept[group, me_year] / base_loss
        stop_ref[:, lanes] = clamp_between(
            loss_ratio - stop_attach_ref[:, lanes], 0.0, stop_width_ref[:, lanes]
        )

    for copy in copies:
        copy.wait_send()


def on_device(sizes, event_loss, event_year, retention, risk_limit, share, member, *terms):
    n_year, n_port, own, groups = sizes
    rows, ports = event_loss.shape
    padded = groups * LANES

    def row(values):
        return values.reshape(1, values.shape[0])

    def term_row(values):
        if padded != own:
            values = jnp.pad(values, (0, padded - own), constant_values=1)
        return row(values)

    vmem = pl.BlockSpec(memory_space=pltpu.VMEM)
    pieces = n_port - 1
    layer_net, stop_loss, tail_mean = pl.pallas_call(
        functools.partial(kernel, sizes),
        name="layers",
        out_shape=(
            jax.ShapeDtypeStruct((YEAR_DEV, padded), jnp.float32),
            jax.ShapeDtypeStruct((YEAR_DEV, padded), jnp.float32),
            jax.ShapeDtypeStruct((1, padded), jnp.float32),
        ),
        in_specs=[vmem] * 12,
        out_specs=(vmem, vmem, vmem),
        scratch_shapes=[
            pltpu.VMEM((rows, ports), jnp.bfloat16),
            pltpu.VMEM((pieces, groups, rows, LANES), jnp.bfloat16),
            pltpu.VMEM((pieces, groups, rows, LANES), jnp.bfloat16),
            pltpu.VMEM((groups, rows, LANES), jnp.float32),
            pltpu.VMEM((groups, rows, LANES), jnp.float32),
            pltpu.VMEM((groups, n_year, YEAR_DEV, LANES), jnp.float32),
            pltpu.SemaphoreType.DMA((pieces, groups)),
            pltpu.SemaphoreType.DMA((pieces, groups)),
            pltpu.SemaphoreType.DMA((groups, n_year)),
            pltpu.SemaphoreType.DMA((groups, n_year)),
        ],
        compiler_params=pltpu.CompilerParams(collective_id=0, has_side_effects=True),
    )(
        event_loss,
        row(event_year),
        row(retention),
        row(risk_limit),
        share.T,
        member.T,
        *[term_row(values) for values in terms],
    )
    return layer_net[:, :own].T, stop_loss[:, :own].T, tail_mean[0, :own]


def solution(mesh):
    n_year, n_port = mesh.shape["year"], mesh.shape["port"]
    own = TREATIES // n_port
    groups = -(-own // LANES)
    return jax.shard_map(
        functools.partial(on_device, (n_year, n_port, own, groups)),
        mesh=mesh,
        in_specs=(
            P("year", "port"),
            P("year"),
            P("port"),
            P("port"),
            P("port", None),
            P("port", None),
            P("port"),
            P("port"),
            P("port"),
            P("port"),
            P("port"),
            P("port"),
        ),
        out_specs=(P("port", "year"), P("port", "year"), P("port")),
        check_vma=False,
    )
```

```python
import functools

import jax
import jax.numpy as jnp
from jax import lax
from jax.experimental import pallas as pl
from jax.experimental.pallas import tpu as pltpu
from jax.sharding import PartitionSpec as P

TREATIES = 1024
YEAR_DEV = 32
TAIL = 16
CHUNKS = 4
LANES = 128
SUBLANES = 8
UNIT_LOSS = 1.0
MESH = pl.DeviceIdType.MESH


def clamp_between(values, lower, upper):
    return jnp.minimum(jnp.maximum(values, lower), upper)


def exchange(items, low, high):
    larger = jnp.maximum(items[low], items[high])
    items[high] = jnp.minimum(items[low], items[high])
    items[low] = larger


def sort_network(count):
    pairs = []
    width = 1
    while width < count:
        step = width
        while step >= 1:
            for start in range(step % width, count - step, 2 * step):
                for offset in range(min(step, count - start - step)):
                    low = start + offset
                    if low // (2 * width) == (low + step) // (2 * width):
                        pairs.append((low, low + step))
            step //= 2
        width *= 2
    return pairs


def sort_falling(items):
    items = list(items)
    for low, high in sort_network(len(items)):
        exchange(items, low, high)
    return items


def merge_largest(first, second, ordered):
    count = len(first)
    items = [jnp.maximum(first[i], second[count - 1 - i]) for i in range(count)]
    step = count // 2
    while ordered and step >= 1:
        for low in range(count):
            if low & step == 0:
                exchange(items, low, low + step)
        step //= 2
    return items


def largest_sum(values):
    rows = values.shape[0]
    tiles = [values[start : start + SUBLANES] for start in range(0, rows, SUBLANES)]
    runs = [sort_falling(tiles[start : start + TAIL]) for start in range(0, len(tiles), TAIL)]
    while len(runs) > 1:
        merged = [
            merge_largest(runs[i], runs[i + 1], True) for i in range(0, len(runs) - 1, 2)
        ]
        runs = merged + runs[len(merged) * 2 :]
    best = runs[0]
    shift = SUBLANES // 2
    while shift >= 1:
        rolled = [pltpu.roll(item, shift, 0) for item in best]
        best = merge_largest(best, rolled, shift > 1)
        shift //= 2
    total = best[0]
    for item in best[1:]:
        total = total + item
    return total[0:1]


def kernel(sizes, *refs):
    sources = refs[:12]
    net_ref, stop_ref, tail_ref = refs[12:15]
    inputs = refs[15:27]
    (
        loss_ref,
        year_ref,
        retention_ref,
        risk_ref,
        share_ref,
        member_ref,
        attach_ref,
        limit_ref,
        reinst_ref,
        rate_ref,
        stop_attach_ref,
        stop_width_ref,
    ) = inputs
    (
        weight,
        ceded,
        sending,
        landing,
        held,
        own_sum,
        kept,
        loss_sem,
        input_sem,
        port_send,
        port_recv,
        year_send,
        year_recv,
    ) = refs[27:]
    n_year, n_port, own, groups = sizes
    rows, ports = loss_ref.shape
    me_port = lax.axis_index("port")
    me_year = lax.axis_index("year")

    barrier = pltpu.get_barrier_semaphore()
    for step in range(1, n_port):
        peer = lax.rem(me_port + step, n_port)
        pl.semaphore_signal(barrier, inc=1, device_id={"port": peer}, device_id_type=MESH)
    for step in range(1, n_year):
        peer = lax.rem(me_year + step, n_year)
        pl.semaphore_signal(barrier, inc=1, device_id={"year": peer}, device_id_type=MESH)

    chunk_rows = rows // CHUNKS

    def chunk(index):
        return slice(index * chunk_rows, (index + 1) * chunk_rows)

    def load(index):
        return pltpu.make_async_copy(sources[index], inputs[index], input_sem.at[index])

    def load_losses(index):
        return pltpu.make_async_copy(
            sources[0].at[chunk(index)], loss_ref.at[chunk(index)], loss_sem.at[index]
        )

    for index in (5, 4):
        load(index).start()
    load_losses(0).start()
    for index in (2, 3):
        load(index).start()
    for index in range(1, CHUNKS):
        load_losses(index).start()
    for index in (1, 6, 7, 8, 9, 10, 11):
        load(index).start()

    def set_weights(dest, group):
        lane = lax.broadcasted_iota(jnp.int32, (LANES, ports), 0) + group * LANES
        treaty = lane + dest * own
        if own % LANES:
            treaty = jnp.where(lane < own, treaty, -1)
        weights = jnp.zeros((LANES, ports), jnp.float32)
        for slot in range(member_ref.shape[0]):
            weights = jnp.where(
                member_ref[slot : slot + 1, :] == treaty,
                share_ref[slot : slot + 1, :].astype(jnp.float32),
                weights,
            )
        weight[...] = weights.astype(jnp.bfloat16)

    def weighted(losses):
        return lax.dot_general(
            losses,
            weight[...],
            (((1,), (1,)), ((), ())),
            preferred_element_type=jnp.float32,
        )

    def product(dest, group):
        set_weights(dest, group)
        return weighted(ceded[...])

    def cede(index):
        load_losses(index).wait()
        if index == 0:
            load(2).wait()
            load(3).wait()
        part = chunk(index)
        ceded[part] = clamp_between(
            loss_ref[part].astype(jnp.float32) - retention_ref[...], 0.0, risk_ref[...]
        ).astype(jnp.bfloat16)

    def port_copy(piece, group, index, device, slot):
        return pltpu.make_async_remote_copy(
            src_ref=sending.at[piece, group, chunk(index)],
            dst_ref=landing.at[slot, group, chunk(index)],
            send_sem=port_send.at[piece, group, index],
            recv_sem=port_recv.at[slot, group, index],
            device_id={"port": device},
            device_id_type=MESH,
        )

    def wait_landed(slot, group, index):
        port_copy(0, group, index, me_port, slot).wait_recv()

    copies = []

    def send(piece, group, index, device, slot):
        copy = port_copy(piece, group, index, device, slot)
        copy.start()
        copies.append(copy)

    def send_first(dest, device, slot):
        load(5).wait()
        load(4).wait()
        set_weights(dest, 0)
        for index in range(CHUNKS):
            cede(index)
            sending[0, 0, chunk(index)] = weighted(ceded[chunk(index)]).astype(jnp.bfloat16)
            if index == 0:
                pl.semaphore_wait(barrier, n_port + n_year - 2)
            send(0, 0, index, device, slot)

    def send_piece(piece, group, dest, device, slot):
        sending[piece, group] = product(dest, group).astype(jnp.bfloat16)
        for index in range(CHUNKS):
            send(piece, group, index, device, slot)

    if n_port == 4:
        is_end = (me_port == 0) | (me_port == 3)
        near = me_port + 1 - 2 * lax.rem(me_port, 2)
        low_half = me_port < 2
        far_end = jnp.where(low_half, 3, 0)
        far_middle = jnp.where(low_half, 2, 1)
        first_dest = jnp.where(is_end, far_middle, far_end)
        first_device = jnp.where(is_end, near, far_end)
        second_dest = jnp.where(is_end, far_end, near)
        last_dest = jnp.where(is_end, near, far_middle)
        last_slot = jnp.where(is_end, 0, 1)
        for group in range(groups):
            if group == 0:
                send_first(first_dest, first_device, 2)
            else:
                send_piece(0, group, first_dest, first_device, 2)
            send_piece(1, group, second_dest, second_dest, jnp.where(is_end, 1, 0))
            held[group] = product(last_dest, group)

            @pl.when(is_end)
            def _():
                sending[2, group] = held[group].astype(jnp.bfloat16)
                for index in range(CHUNKS):
                    port_copy(2, group, index, last_dest, last_slot).start()

        for group in range(groups):
            own_sum[group] = product(me_port, group)
        for group in range(groups):

            @pl.when(jnp.logical_not(is_end))
            def _():
                for index in range(CHUNKS):
                    wait_landed(2, group, index)
                    part = chunk(index)
                    sending[2, group, part] = (
                        held[group, part] + landing[2, group, part].astype(jnp.float32)
                    ).astype(jnp.bfloat16)
                    port_copy(2, group, index, last_dest, last_slot).start()

            for index in range(CHUNKS):
                copies.append(port_copy(2, group, index, last_dest, last_slot))

    else:
        for group in range(groups):
            for step in range(1, n_port):
                dest = lax.rem(me_port + step, n_port)
                if group == 0 and step == 1:
                    send_first(dest, dest, 0)
                else:
                    send_piece(step - 1, group, dest, dest, step - 1)
        for group in range(groups):
            own_sum[group] = product(me_port, group)
    for index in (1, 6, 7, 8, 9, 10, 11):
        load(index).wait()

    local_year = year_ref[...] - me_year * YEAR_DEV
    hits = (
        (local_year == lax.broadcasted_iota(jnp.int32, (YEAR_DEV, rows), 0))
        .astype(jnp.float32)
        .astype(jnp.bfloat16)
    )

    def split_dot(values):
        upper = values.astype(jnp.bfloat16)
        lower = (values - upper.astype(jnp.float32)).astype(jnp.bfloat16)
        return jnp.dot(hits, upper, preferred_element_type=jnp.float32) + jnp.dot(
            hits, lower, preferred_element_type=jnp.float32
        )

    def year_copy(step, group):
        return pltpu.make_async_remote_copy(
            src_ref=kept.at[group, me_year],
            dst_ref=kept.at[group, me_year],
            send_sem=year_send.at[group, step - 1],
            recv_sem=year_recv.at[group, me_year],
            device_id={"year": lax.rem(me_year + step, n_year)},
            device_id_type=MESH,
        )

    for group in range(groups):
        lanes = slice(group * LANES, (group + 1) * LANES)
        event_treaty = own_sum[group]
        if n_port == 4:
            for index in range(CHUNKS):
                wait_landed(0, group, index)
                wait_landed(1, group, index)

            @pl.when(is_end)
            def _():
                for index in range(CHUNKS):
                    wait_landed(2, group, index)

            event_treaty = event_treaty + landing[0, group].astype(jnp.float32)
            event_treaty = event_treaty + landing[1, group].astype(jnp.float32)
            event_treaty = event_treaty + jnp.where(
                is_end, landing[2, group].astype(jnp.float32), 0.0
            )
        else:
            for slot in range(n_port - 1):
                for index in range(CHUNKS):
                    wait_landed(slot, group, index)
                event_treaty = event_treaty + landing[slot, group].astype(jnp.float32)
        attach = attach_ref[:, lanes].astype(jnp.float32) * UNIT_LOSS
        limit_loss = limit_ref[:, lanes].astype(jnp.float32) * UNIT_LOSS
        recovered = clamp_between(event_treaty - attach, 0.0, limit_loss)
        retained = event_treaty - recovered
        yearly = split_dot(jnp.concatenate((recovered, retained), 1))
        annual = yearly[:, :LANES]
        kept[group, me_year] = yearly[:, LANES:]
        for step in range(1, n_year):
            copy = year_copy(step, group)
            copy.start()
            copies.append(copy)
        reinstated = reinst_ref[:, lanes].astype(jnp.float32)
        layer_paid = jnp.minimum(annual, (1.0 + reinstated) * limit_loss)
        net_ref[:, lanes] = (
            layer_paid
            - rate_ref[:, lanes] * jnp.minimum(layer_paid, reinstated * limit_loss)
        ) / limit_loss

    for group in range(groups):
        lanes = slice(group * LANES, (group + 1) * LANES)
        for step in range(1, n_year):
            source = lax.rem(me_year + step, n_year)
            pltpu.make_async_remote_copy(
                src_ref=kept.at[group, source],
                dst_ref=kept.at[group, source],
                send_sem=year_send.at[group, step - 1],
                recv_sem=year_recv.at[group, source],
                device_id={"year": source},
                device_id_type=MESH,
            ).wait_recv()
        every = kept[group].reshape(n_year * YEAR_DEV, LANES)
        base_loss = UNIT_LOSS + jnp.sum(every, axis=0, keepdims=True) / (n_year * YEAR_DEV)
        tail_ref[:, lanes] = largest_sum(every) / base_loss / TAIL
        loss_ratio = kept[group, me_year] / base_loss
        stop_ref[:, lanes] = clamp_between(
            loss_ratio - stop_attach_ref[:, lanes], 0.0, stop_width_ref[:, lanes]
        )

    for copy in copies:
        copy.wait_send()


def put_out(*refs):
    results, outputs, sem = refs[:3], refs[3:6], refs[6]
    moves = [
        pltpu.make_async_copy(result, output, sem.at[index])
        for index, (result, output) in enumerate(zip(results, outputs))
    ]
    for move in moves:
        move.start()
    for move in moves:
        move.wait()


def on_device(sizes, event_loss, event_year, retention, risk_limit, share, member, *terms):
    n_year, n_port, own, groups = sizes
    rows, ports = event_loss.shape
    padded = groups * LANES

    def row(values):
        return values.reshape(1, values.shape[0])

    def term_row(values):
        if padded != own:
            values = jnp.pad(values, (0, padded - own), constant_values=1)
        return row(values)

    operands = [
        event_loss,
        row(event_year),
        row(retention),
        row(risk_limit),
        share.T,
        member.T,
        *[term_row(values) for values in terms],
    ]
    anywhere = pl.BlockSpec(memory_space=pl.ANY)
    vmem = pl.BlockSpec(memory_space=pltpu.VMEM)
    pieces = n_port - 1
    shapes = [(YEAR_DEV, padded), (YEAR_DEV, padded), (1, padded)]
    results = pl.pallas_call(
        functools.partial(kernel, sizes),
        name="layers",
        out_shape=[pltpu.VMEM(shape, jnp.float32) for shape in shapes],
        in_specs=[anywhere] * len(operands),
        out_specs=[vmem] * len(shapes),
        scratch_shapes=[
            *[pltpu.VMEM(operand.shape, operand.dtype) for operand in operands],
            pltpu.VMEM((LANES, ports), jnp.bfloat16),
            pltpu.VMEM((rows, ports), jnp.bfloat16),
            pltpu.VMEM((pieces, groups, rows, LANES), jnp.bfloat16),
            pltpu.VMEM((pieces, groups, rows, LANES), jnp.bfloat16),
            pltpu.VMEM((groups, rows, LANES), jnp.float32),
            pltpu.VMEM((groups, rows, LANES), jnp.float32),
            pltpu.VMEM((groups, n_year, YEAR_DEV, LANES), jnp.float32),
            pltpu.SemaphoreType.DMA((CHUNKS,)),
            pltpu.SemaphoreType.DMA((len(operands),)),
            pltpu.SemaphoreType.DMA((pieces, groups, CHUNKS)),
            pltpu.SemaphoreType.DMA((pieces, groups, CHUNKS)),
            pltpu.SemaphoreType.DMA((groups, n_year)),
            pltpu.SemaphoreType.DMA((groups, n_year)),
        ],
        compiler_params=pltpu.CompilerParams(collective_id=0, has_side_effects=True),
    )(*operands)
    layer_net, stop_loss, tail_mean = pl.pallas_call(
        put_out,
        name="put_out",
        out_shape=[jax.ShapeDtypeStruct(shape, jnp.float32) for shape in shapes],
        in_specs=[anywhere] * len(shapes),
        out_specs=[anywhere] * len(shapes),
        scratch_shapes=[pltpu.SemaphoreType.DMA((len(shapes),))],
    )(*[pltpu.with_memory_space_constraint(value, pltpu.VMEM) for value in results])
    return layer_net[:, :own].T, stop_loss[:, :own].T, tail_mean[0, :own]


def solution(mesh):
    n_year, n_port = mesh.shape["year"], mesh.shape["port"]
    own = TREATIES // n_port
    groups = -(-own // LANES)
    return jax.shard_map(
        functools.partial(on_device, (n_year, n_port, own, groups)),
        mesh=mesh,
        in_specs=(
            P("year", "port"),
            P("year"),
            P("port"),
            P("port"),
            P("port", None),
            P("port", None),
            P("port"),
            P("port"),
            P("port"),
            P("port"),
            P("port"),
            P("port"),
        ),
        out_specs=(P("port", "year"), P("port", "year"), P("port")),
        check_vma=False,
    )
```

```python
import functools

import jax
import jax.numpy as jnp
from jax import lax
from jax.experimental import pallas as pl
from jax.experimental.pallas import tpu as pltpu
from jax.sharding import PartitionSpec as P

TREATIES = 1024
YEAR_DEV = 32
TAIL = 16
CHUNKS = 4
LANES = 128
SUBLANES = 8
UNIT_LOSS = 1.0
MESH = pl.DeviceIdType.MESH


def clamp_between(values, lower, upper):
    return jnp.minimum(jnp.maximum(values, lower), upper)


def exchange(items, low, high):
    larger = jnp.maximum(items[low], items[high])
    items[high] = jnp.minimum(items[low], items[high])
    items[low] = larger


def sort_network(count):
    pairs = []
    width = 1
    while width < count:
        step = width
        while step >= 1:
            for start in range(step % width, count - step, 2 * step):
                for offset in range(min(step, count - start - step)):
                    low = start + offset
                    if low // (2 * width) == (low + step) // (2 * width):
                        pairs.append((low, low + step))
            step //= 2
        width *= 2
    return pairs


def sort_falling(items):
    items = list(items)
    for low, high in sort_network(len(items)):
        exchange(items, low, high)
    return items


def merge_largest(first, second, ordered):
    count = len(first)
    items = [jnp.maximum(first[i], second[count - 1 - i]) for i in range(count)]
    step = count // 2
    while ordered and step >= 1:
        for low in range(count):
            if low & step == 0:
                exchange(items, low, low + step)
        step //= 2
    return items


def largest_sum(values):
    rows = values.shape[0]
    tiles = [values[start : start + SUBLANES] for start in range(0, rows, SUBLANES)]
    runs = [sort_falling(tiles[start : start + TAIL]) for start in range(0, len(tiles), TAIL)]
    while len(runs) > 1:
        merged = [
            merge_largest(runs[i], runs[i + 1], True) for i in range(0, len(runs) - 1, 2)
        ]
        runs = merged + runs[len(merged) * 2 :]
    best = runs[0]
    shift = SUBLANES // 2
    while shift >= 1:
        rolled = [pltpu.roll(item, shift, 0) for item in best]
        best = merge_largest(best, rolled, shift > 1)
        shift //= 2
    total = best[0]
    for item in best[1:]:
        total = total + item
    return total[0:1]


def kernel(sizes, *refs):
    sources = refs[:12]
    net_ref, stop_ref, tail_ref = refs[12:15]
    inputs = refs[15:27]
    (
        loss_ref,
        year_ref,
        retention_ref,
        risk_ref,
        share_ref,
        member_ref,
        attach_ref,
        limit_ref,
        reinst_ref,
        rate_ref,
        stop_attach_ref,
        stop_width_ref,
    ) = inputs
    (
        terms,
        given,
        adopted,
        weight,
        ceded,
        sending,
        landing,
        held,
        own_sum,
        kept,
        hand_sem,
        loss_sem,
        input_sem,
        port_send,
        port_recv,
        year_send,
        year_recv,
    ) = refs[27:]
    n_year, n_port, own, groups = sizes
    rows, ports = loss_ref.shape
    me_port = lax.axis_index("port")
    me_year = lax.axis_index("year")

    barrier = pltpu.get_barrier_semaphore()
    for step in range(1, n_port):
        peer = lax.rem(me_port + step, n_port)
        pl.semaphore_signal(barrier, inc=1, device_id={"port": peer}, device_id_type=MESH)
    for step in range(1, n_year):
        peer = lax.rem(me_year + step, n_year)
        pl.semaphore_signal(barrier, inc=1, device_id={"year": peer}, device_id_type=MESH)

    chunk_rows = rows // CHUNKS

    def chunk(index):
        return slice(index * chunk_rows, (index + 1) * chunk_rows)

    def load(index):
        return pltpu.make_async_copy(sources[index], inputs[index], input_sem.at[index])

    def load_losses(index):
        return pltpu.make_async_copy(
            sources[0].at[chunk(index)], loss_ref.at[chunk(index)], loss_sem.at[index]
        )

    for index in (5, 4):
        load(index).start()
    load_losses(0).start()
    for index in (2, 3):
        load(index).start()
    for index in range(1, CHUNKS):
        load_losses(index).start()
    for index in (1, 6, 7, 8, 9, 10, 11):
        load(index).start()

    def set_weights(dest, group):
        lane = lax.broadcasted_iota(jnp.int32, (LANES, ports), 0) + group * LANES
        treaty = lane + dest * own
        if own % LANES:
            treaty = jnp.where(lane < own, treaty, -1)
        weights = jnp.zeros((LANES, ports), jnp.float32)
        for slot in range(member_ref.shape[0]):
            weights = jnp.where(
                member_ref[slot : slot + 1, :] == treaty,
                share_ref[slot : slot + 1, :].astype(jnp.float32),
                weights,
            )
        weight[...] = weights.astype(jnp.bfloat16)

    def weighted(losses):
        return lax.dot_general(
            losses,
            weight[...],
            (((1,), (1,)), ((), ())),
            preferred_element_type=jnp.float32,
        )

    def product(dest, group):
        set_weights(dest, group)
        return weighted(ceded[...])

    def cede(index):
        load_losses(index).wait()
        if index == 0:
            load(2).wait()
            load(3).wait()
        part = chunk(index)
        ceded[part] = clamp_between(
            loss_ref[part].astype(jnp.float32) - retention_ref[...], 0.0, risk_ref[...]
        ).astype(jnp.bfloat16)

    def port_copy(piece, index, device, slot):
        return pltpu.make_async_remote_copy(
            src_ref=sending.at[piece, chunk(index)],
            dst_ref=landing.at[slot, chunk(index)],
            send_sem=port_send.at[piece, index],
            recv_sem=port_recv.at[slot, index],
            device_id={"port": device},
            device_id_type=MESH,
        )

    def hand_copy(which, source, target, device):
        return pltpu.make_async_remote_copy(
            src_ref=source,
            dst_ref=target,
            send_sem=hand_sem.at[which, 0],
            recv_sem=hand_sem.at[which, 1],
            device_id={"port": device},
            device_id_type=MESH,
        )

    def wait_landed(slot, index):
        port_copy(0, index, me_port, slot).wait_recv()

    def send(copies, piece, index, device, slot):
        copy = port_copy(piece, index, device, slot)
        copy.start()
        copies.append(copy)

    def send_first(copies, dest, group, device, slot):
        load(5).wait()
        load(4).wait()
        set_weights(dest, group)
        for index in range(CHUNKS):
            cede(index)
            sending[0, chunk(index)] = weighted(ceded[chunk(index)]).astype(jnp.bfloat16)
            if index == 0:
                pl.semaphore_wait(barrier, n_port + n_year - 2)
            send(copies, 0, index, device, slot)

    def send_piece(copies, piece, dest, group, device, slot):
        sending[piece] = product(dest, group).astype(jnp.bfloat16)
        for index in range(CHUNKS):
            send(copies, piece, index, device, slot)

    def merge(copies, store, landed, piece, device, slot):
        for index in range(CHUNKS):
            wait_landed(landed, index)
            part = chunk(index)
            sending[piece, part] = (
                held[store, part] + landing[landed, part].astype(jnp.float32)
            ).astype(jnp.bfloat16)
            send(copies, piece, index, device, slot)

    def gather_terms():
        for index in (1, 6, 7, 8, 9, 10, 11):
            load(index).wait()
        for group in range(groups):
            for place, ref in enumerate(inputs[6:12]):
                terms[group, place : place + 1, :] = ref[:, lanes_of(group)].astype(jnp.float32)
            terms[group, 6:8, :] = jnp.ones((2, LANES), jnp.float32)

    def lanes_of(group):
        return slice(group * LANES, (group + 1) * LANES)

    def term(group, place):
        return terms[group, place : place + 1, :]

    def split_dot(values):
        local_year = year_ref[...] - me_year * YEAR_DEV
        hits = (
            (local_year == lax.broadcasted_iota(jnp.int32, (YEAR_DEV, rows), 0))
            .astype(jnp.float32)
            .astype(jnp.bfloat16)
        )
        upper = values.astype(jnp.bfloat16)
        lower = (values - upper.astype(jnp.float32)).astype(jnp.bfloat16)
        return jnp.dot(hits, upper, preferred_element_type=jnp.float32) + jnp.dot(
            hits, lower, preferred_element_type=jnp.float32
        )

    def year_copy(place, step, owner):
        return pltpu.make_async_remote_copy(
            src_ref=kept.at[place, owner],
            dst_ref=kept.at[place, owner],
            send_sem=year_send.at[place, step - 1],
            recv_sem=year_recv.at[place, owner],
            device_id={"year": lax.rem(me_year + step, n_year)},
            device_id_type=MESH,
        )

    def year_stage(copies, place, slots, group):
        event_treaty = own_sum[place]
        for slot in slots:
            for index in range(CHUNKS):
                wait_landed(slot, index)
            event_treaty = event_treaty + landing[slot].astype(jnp.float32)
        attach = term(group, 0) * UNIT_LOSS
        limit_loss = term(group, 1) * UNIT_LOSS
        recovered = clamp_between(event_treaty - attach, 0.0, limit_loss)
        retained = event_treaty - recovered
        yearly = split_dot(jnp.concatenate((recovered, retained), 1))
        annual = yearly[:, :LANES]
        kept[place, me_year] = yearly[:, LANES:]
        for step in range(1, n_year):
            copy = year_copy(place, step, me_year)
            copy.start()
            copies.append(copy)
        reinstated = term(group, 2)
        layer_paid = jnp.minimum(annual, (1.0 + reinstated) * limit_loss)
        return (
            layer_paid - term(group, 3) * jnp.minimum(layer_paid, reinstated * limit_loss)
        ) / limit_loss

    def last_stage(place, group):
        for step in range(1, n_year):
            year_copy(place, step, lax.rem(me_year + step, n_year)).wait_recv()
        every = kept[place].reshape(n_year * YEAR_DEV, LANES)
        base_loss = UNIT_LOSS + jnp.sum(every, axis=0, keepdims=True) / (n_year * YEAR_DEV)
        tail = largest_sum(every) / base_loss / TAIL
        loss_ratio = kept[place, me_year] / base_loss
        return clamp_between(loss_ratio - term(group, 4), 0.0, term(group, 5)), tail

    def finish(copies):
        for copy in copies:
            copy.wait_send()

    if balanced(n_port, groups):
        is_end = (me_port == 0) | (me_port == 3)
        low_half = me_port < 2
        near_end = jnp.where(low_half, 0, 3)
        near_middle = jnp.where(low_half, 1, 2)
        far_end = 3 - near_end
        far_middle = 3 - near_middle

        @pl.when(is_end)
        def _():
            copies = []
            send_first(copies, far_middle, 0, near_middle, 0)
            send_piece(copies, 1, far_end, 0, near_middle, 1)
            send_piece(copies, 2, far_end, 1, near_middle, 2)
            send_piece(copies, 3, far_middle, 1, near_middle, 3)
            send_piece(copies, 4, near_middle, 1, near_middle, 4)
            own_sum[0] = product(near_middle, 0)
            own_sum[1] = product(near_end, 0)
            own_sum[2] = product(near_end, 1)
            gather_terms()
            hand_copy(0, terms.at[0], terms.at[groups], me_port).wait_recv()
            adopted_net = year_stage(copies, 0, (0,), groups)
            net_ref[:, lanes_of(0)] = year_stage(copies, 1, (1, 2), 0)
            adopted_stop, adopted_tail = last_stage(0, groups)
            given[0:YEAR_DEV] = adopted_net
            given[YEAR_DEV : 2 * YEAR_DEV] = adopted_stop
            given[2 * YEAR_DEV :] = jnp.broadcast_to(adopted_tail, (SUBLANES, LANES))
            hand_over = hand_copy(1, given, adopted, near_middle)
            hand_over.start()
            copies.append(hand_over)
            net_ref[:, lanes_of(1)] = year_stage(copies, 2, (3, 4), 1)
            for group in range(groups):
                stop_loss, tail = last_stage(1 + group, group)
                stop_ref[:, lanes_of(group)] = stop_loss
                tail_ref[:, lanes_of(group)] = tail
            finish(copies)

        @pl.when(jnp.logical_not(is_end))
        def _():
            copies = []
            send_first(copies, near_end, 0, near_end, 2)
            gather_terms()
            hand_over = hand_copy(0, terms.at[0], terms.at[groups], near_end)
            hand_over.start()
            copies.append(hand_over)
            send_piece(copies, 1, near_end, 1, near_end, 4)
            held[0] = product(far_middle, 0)
            held[1] = product(far_end, 0)
            held[2] = product(near_middle, 0)
            merge(copies, 0, 0, 2, far_middle, 5)
            held[3] = product(far_end, 1)
            held[4] = product(far_middle, 1)
            merge(copies, 1, 1, 3, far_end, 1)
            own_sum[0] = product(near_middle, 1)
            merge(copies, 2, 5, 4, near_end, 0)
            merge(copies, 3, 2, 5, far_end, 3)
            merge(copies, 4, 3, 6, far_middle, 6)
            net_ref[:, lanes_of(1)] = year_stage(copies, 0, (6, 4), 1)
            hand_copy(1, given, adopted, me_port).wait_recv()
            net_ref[:, lanes_of(0)] = adopted[0:YEAR_DEV]
            stop_ref[:, lanes_of(0)] = adopted[YEAR_DEV : 2 * YEAR_DEV]
            tail_ref[:, lanes_of(0)] = adopted[2 * YEAR_DEV : 2 * YEAR_DEV + 1]
            stop_loss, tail = last_stage(0, 1)
            stop_ref[:, lanes_of(1)] = stop_loss
            tail_ref[:, lanes_of(1)] = tail
            finish(copies)

    else:
        copies = []
        for group in range(groups):
            for step in range(1, n_port):
                dest = lax.rem(me_port + step, n_port)
                slot = (step - 1) * groups + group
                if slot == 0:
                    send_first(copies, dest, group, dest, slot)
                else:
                    send_piece(copies, slot, dest, group, dest, slot)
        for group in range(groups):
            own_sum[group] = product(me_port, group)
        gather_terms()
        for group in range(groups):
            slots = [step * groups + group for step in range(n_port - 1)]
            net_ref[:, lanes_of(group)] = year_stage(copies, group, slots, group)
        for group in range(groups):
            stop_loss, tail = last_stage(group, group)
            stop_ref[:, lanes_of(group)] = stop_loss
            tail_ref[:, lanes_of(group)] = tail
        finish(copies)


def balanced(n_port, groups):
    return n_port == 4 and groups == 2


def put_out(*refs):
    results, outputs, sem = refs[:3], refs[3:6], refs[6]
    moves = [
        pltpu.make_async_copy(result, output, sem.at[index])
        for index, (result, output) in enumerate(zip(results, outputs))
    ]
    for move in moves:
        move.start()
    for move in moves:
        move.wait()


def on_device(sizes, event_loss, event_year, retention, risk_limit, share, member, *terms):
    n_year, n_port, own, groups = sizes
    rows, ports = event_loss.shape
    padded = groups * LANES

    def row(values):
        return values.reshape(1, values.shape[0])

    def term_row(values):
        if padded != own:
            values = jnp.pad(values, (0, padded - own), constant_values=1)
        return row(values)

    operands = [
        event_loss,
        row(event_year),
        row(retention),
        row(risk_limit),
        share.T,
        member.T,
        *[term_row(values) for values in terms],
    ]
    anywhere = pl.BlockSpec(memory_space=pl.ANY)
    vmem = pl.BlockSpec(memory_space=pltpu.VMEM)
    if balanced(n_port, groups):
        pieces, places, stores = 7, groups + 1, 5
    else:
        pieces, places, stores = (n_port - 1) * groups, groups, 1
    shapes = [(YEAR_DEV, padded), (YEAR_DEV, padded), (1, padded)]
    results = pl.pallas_call(
        functools.partial(kernel, sizes),
        name="layers",
        out_shape=[pltpu.VMEM(shape, jnp.float32) for shape in shapes],
        in_specs=[anywhere] * len(operands),
        out_specs=[vmem] * len(shapes),
        scratch_shapes=[
            *[pltpu.VMEM(operand.shape, operand.dtype) for operand in operands],
            pltpu.VMEM((groups + 1, SUBLANES, LANES), jnp.float32),
            pltpu.VMEM((2 * YEAR_DEV + SUBLANES, LANES), jnp.float32),
            pltpu.VMEM((2 * YEAR_DEV + SUBLANES, LANES), jnp.float32),
            pltpu.VMEM((LANES, ports), jnp.bfloat16),
            pltpu.VMEM((rows, ports), jnp.bfloat16),
            pltpu.VMEM((pieces, rows, LANES), jnp.bfloat16),
            pltpu.VMEM((pieces, rows, LANES), jnp.bfloat16),
            pltpu.VMEM((stores, rows, LANES), jnp.float32),
            pltpu.VMEM((places, rows, LANES), jnp.float32),
            pltpu.VMEM((places, n_year, YEAR_DEV, LANES), jnp.float32),
            pltpu.SemaphoreType.DMA((2, 2)),
            pltpu.SemaphoreType.DMA((CHUNKS,)),
            pltpu.SemaphoreType.DMA((len(operands),)),
            pltpu.SemaphoreType.DMA((pieces, CHUNKS)),
            pltpu.SemaphoreType.DMA((pieces, CHUNKS)),
            pltpu.SemaphoreType.DMA((places, n_year)),
            pltpu.SemaphoreType.DMA((places, n_year)),
        ],
        compiler_params=pltpu.CompilerParams(collective_id=0, has_side_effects=True),
    )(*operands)
    layer_net, stop_loss, tail_mean = pl.pallas_call(
        put_out,
        name="put_out",
        out_shape=[jax.ShapeDtypeStruct(shape, jnp.float32) for shape in shapes],
        in_specs=[anywhere] * len(shapes),
        out_specs=[anywhere] * len(shapes),
        scratch_shapes=[pltpu.SemaphoreType.DMA((len(shapes),))],
    )(*[pltpu.with_memory_space_constraint(value, pltpu.VMEM) for value in results])
    return layer_net[:, :own].T, stop_loss[:, :own].T, tail_mean[0, :own]


def solution(mesh):
    n_year, n_port = mesh.shape["year"], mesh.shape["port"]
    own = TREATIES // n_port
    groups = -(-own // LANES)
    return jax.shard_map(
        functools.partial(on_device, (n_year, n_port, own, groups)),
        mesh=mesh,
        in_specs=(
            P("year", "port"),
            P("year"),
            P("port"),
            P("port"),
            P("port", None),
            P("port", None),
            P("port"),
            P("port"),
            P("port"),
            P("port"),
            P("port"),
            P("port"),
        ),
        out_specs=(P("port", "year"), P("port", "year"), P("port")),
        check_vma=False,
    )
```

```python
import functools

import jax
import jax.numpy as jnp
from jax import lax
from jax.experimental import pallas as pl
from jax.experimental.pallas import tpu as pltpu
from jax.sharding import PartitionSpec as P

TREATIES = 1024
YEAR_DEV = 32
TAIL = 16
CHUNKS = 4
LANES = 128
SUBLANES = 8
UNIT_LOSS = 1.0
MESH = pl.DeviceIdType.MESH


def clamp_between(values, lower, upper):
    return jnp.minimum(jnp.maximum(values, lower), upper)


def exchange(items, low, high):
    larger = jnp.maximum(items[low], items[high])
    items[high] = jnp.minimum(items[low], items[high])
    items[low] = larger


def sort_network(count):
    pairs = []
    width = 1
    while width < count:
        step = width
        while step >= 1:
            for start in range(step % width, count - step, 2 * step):
                for offset in range(min(step, count - start - step)):
                    low = start + offset
                    if low // (2 * width) == (low + step) // (2 * width):
                        pairs.append((low, low + step))
            step //= 2
        width *= 2
    return pairs


def sort_falling(items):
    items = list(items)
    for low, high in sort_network(len(items)):
        exchange(items, low, high)
    return items


def merge_largest(first, second, ordered):
    count = len(first)
    items = [jnp.maximum(first[i], second[count - 1 - i]) for i in range(count)]
    step = count // 2
    while ordered and step >= 1:
        for low in range(count):
            if low & step == 0:
                exchange(items, low, low + step)
        step //= 2
    return items


def largest_sum(values):
    rows = values.shape[0]
    tiles = [values[start : start + SUBLANES] for start in range(0, rows, SUBLANES)]
    runs = [sort_falling(tiles[start : start + TAIL]) for start in range(0, len(tiles), TAIL)]
    while len(runs) > 1:
        merged = [
            merge_largest(runs[i], runs[i + 1], True) for i in range(0, len(runs) - 1, 2)
        ]
        runs = merged + runs[len(merged) * 2 :]
    best = runs[0]
    shift = SUBLANES // 2
    while shift >= 1:
        rolled = [pltpu.roll(item, shift, 0) for item in best]
        best = merge_largest(best, rolled, shift > 1)
        shift //= 2
    total = best[0]
    for item in best[1:]:
        total = total + item
    return total[0:1]


def kernel(sizes, *refs):
    sources = refs[:12]
    net_ref, stop_ref, tail_ref = refs[12:15]
    inputs = refs[15:27]
    (
        loss_ref,
        year_ref,
        retention_ref,
        risk_ref,
        share_ref,
        member_ref,
        attach_ref,
        limit_ref,
        reinst_ref,
        rate_ref,
        stop_attach_ref,
        stop_width_ref,
    ) = inputs
    (
        weight,
        ceded,
        sending,
        landing,
        held,
        own_sum,
        kept,
        loss_sem,
        input_sem,
        port_send,
        port_recv,
        year_send,
        year_recv,
    ) = refs[27:]
    n_year, n_port, own, groups = sizes
    rows, ports = loss_ref.shape
    me_port = lax.axis_index("port")
    me_year = lax.axis_index("year")

    chunk_rows = rows // CHUNKS

    def chunk(index):
        return slice(index * chunk_rows, (index + 1) * chunk_rows)

    def load(index):
        return pltpu.make_async_copy(sources[index], inputs[index], input_sem.at[index])

    def load_losses(index):
        return pltpu.make_async_copy(
            sources[0].at[chunk(index)], loss_ref.at[chunk(index)], loss_sem.at[index]
        )

    for index in (5, 4):
        load(index).start()
    load_losses(0).start()
    for index in (2, 3):
        load(index).start()
    for index in range(1, CHUNKS):
        load_losses(index).start()
    for index in (1, 6, 7, 8, 9, 10, 11):
        load(index).start()

    barrier = pltpu.get_barrier_semaphore()
    for step in range(1, n_port):
        peer = lax.rem(me_port + step, n_port)
        pl.semaphore_signal(barrier, inc=1, device_id={"port": peer}, device_id_type=MESH)
    for step in range(1, n_year):
        peer = lax.rem(me_year + step, n_year)
        pl.semaphore_signal(barrier, inc=1, device_id={"year": peer}, device_id_type=MESH)

    def set_weights(dest, group):
        lane = lax.broadcasted_iota(jnp.int32, (LANES, ports), 0) + group * LANES
        treaty = lane + dest * own
        if own % LANES:
            treaty = jnp.where(lane < own, treaty, -1)
        weights = jnp.zeros((LANES, ports), jnp.float32)
        for slot in range(member_ref.shape[0]):
            weights = jnp.where(
                member_ref[slot : slot + 1, :] == treaty,
                share_ref[slot : slot + 1, :].astype(jnp.float32),
                weights,
            )
        weight[...] = weights.astype(jnp.bfloat16)

    def weighted(losses):
        return lax.dot_general(
            losses,
            weight[...],
            (((1,), (1,)), ((), ())),
            preferred_element_type=jnp.float32,
        )

    def product(dest, group):
        set_weights(dest, group)
        return weighted(ceded[...])

    def cede(index):
        load_losses(index).wait()
        if index == 0:
            load(2).wait()
            load(3).wait()
        part = chunk(index)
        ceded[part] = clamp_between(
            loss_ref[part].astype(jnp.float32) - retention_ref[...], 0.0, risk_ref[...]
        ).astype(jnp.bfloat16)

    def port_copy(piece, group, index, device, slot):
        return pltpu.make_async_remote_copy(
            src_ref=sending.at[piece, group, chunk(index)],
            dst_ref=landing.at[slot, group, chunk(index)],
            send_sem=port_send.at[piece, group, index],
            recv_sem=port_recv.at[slot, group, index],
            device_id={"port": device},
            device_id_type=MESH,
        )

    def wait_landed(slot, group, index):
        port_copy(0, group, index, me_port, slot).wait_recv()

    copies = []

    def send(piece, group, index, device, slot):
        copy = port_copy(piece, group, index, device, slot)
        copy.start()
        copies.append(copy)

    def send_first(dest, device, slot):
        load(5).wait()
        load(4).wait()
        set_weights(dest, 0)
        for index in range(CHUNKS):
            cede(index)
            sending[0, 0, chunk(index)] = weighted(ceded[chunk(index)]).astype(jnp.bfloat16)
            if index == 0:
                pl.semaphore_wait(barrier, n_port + n_year - 2)
            send(0, 0, index, device, slot)

    def send_piece(piece, group, dest, device, slot):
        sending[piece, group] = product(dest, group).astype(jnp.bfloat16)
        for index in range(CHUNKS):
            send(piece, group, index, device, slot)

    if n_port == 4:
        is_end = (me_port == 0) | (me_port == 3)
        near = me_port + 1 - 2 * lax.rem(me_port, 2)
        low_half = me_port < 2
        far_end = jnp.where(low_half, 3, 0)
        far_middle = jnp.where(low_half, 2, 1)
        first_dest = jnp.where(is_end, far_middle, far_end)
        first_device = jnp.where(is_end, near, far_end)
        second_dest = jnp.where(is_end, far_end, near)
        last_dest = jnp.where(is_end, near, far_middle)
        last_slot = jnp.where(is_end, 0, 1)
        for group in range(groups):
            if group == 0:
                send_first(first_dest, first_device, 2)
            else:
                send_piece(0, group, first_dest, first_device, 2)
        for group in range(groups):
            send_piece(1, group, second_dest, second_dest, jnp.where(is_end, 1, 0))
            held[group] = product(last_dest, group)

            @pl.when(is_end)
            def _():
                sending[2, group] = held[group].astype(jnp.bfloat16)
                for index in range(CHUNKS):
                    port_copy(2, group, index, last_dest, last_slot).start()

        for group in range(groups):
            own_sum[group] = product(me_port, group)
        for group in range(groups):

            @pl.when(jnp.logical_not(is_end))
            def _():
                for index in range(CHUNKS):
                    wait_landed(2, group, index)
                    part = chunk(index)
                    sending[2, group, part] = (
                        held[group, part] + landing[2, group, part].astype(jnp.float32)
                    ).astype(jnp.bfloat16)
                    port_copy(2, group, index, last_dest, last_slot).start()

            for index in range(CHUNKS):
                copies.append(port_copy(2, group, index, last_dest, last_slot))

    else:
        for group in range(groups):
            for step in range(1, n_port):
                dest = lax.rem(me_port + step, n_port)
                if group == 0 and step == 1:
                    send_first(dest, dest, 0)
                else:
                    send_piece(step - 1, group, dest, dest, step - 1)
        for group in range(groups):
            own_sum[group] = product(me_port, group)
    for index in (1, 6, 7, 8, 9, 10, 11):
        load(index).wait()

    local_year = year_ref[...] - me_year * YEAR_DEV
    hits = (
        (local_year == lax.broadcasted_iota(jnp.int32, (YEAR_DEV, rows), 0))
        .astype(jnp.float32)
        .astype(jnp.bfloat16)
    )

    def split_dot(values):
        upper = values.astype(jnp.bfloat16)
        lower = (values - upper.astype(jnp.float32)).astype(jnp.bfloat16)
        return jnp.dot(hits, upper, preferred_element_type=jnp.float32) + jnp.dot(
            hits, lower, preferred_element_type=jnp.float32
        )

    def year_copy(step, group):
        return pltpu.make_async_remote_copy(
            src_ref=kept.at[group, me_year],
            dst_ref=kept.at[group, me_year],
            send_sem=year_send.at[group, step - 1],
            recv_sem=year_recv.at[group, me_year],
            device_id={"year": lax.rem(me_year + step, n_year)},
            device_id_type=MESH,
        )

    for group in range(groups):
        lanes = slice(group * LANES, (group + 1) * LANES)
        event_treaty = own_sum[group]
        if n_port == 4:
            for index in range(CHUNKS):
                wait_landed(0, group, index)
                wait_landed(1, group, index)

            @pl.when(is_end)
            def _():
                for index in range(CHUNKS):
                    wait_landed(2, group, index)

            event_treaty = event_treaty + landing[0, group].astype(jnp.float32)
            event_treaty = event_treaty + landing[1, group].astype(jnp.float32)
            event_treaty = event_treaty + jnp.where(
                is_end, landing[2, group].astype(jnp.float32), 0.0
            )
        else:
            for slot in range(n_port - 1):
                for index in range(CHUNKS):
                    wait_landed(slot, group, index)
                event_treaty = event_treaty + landing[slot, group].astype(jnp.float32)
        attach = attach_ref[:, lanes].astype(jnp.float32) * UNIT_LOSS
        limit_loss = limit_ref[:, lanes].astype(jnp.float32) * UNIT_LOSS
        recovered = clamp_between(event_treaty - attach, 0.0, limit_loss)
        retained = event_treaty - recovered
        yearly = split_dot(jnp.concatenate((recovered, retained), 1))
        annual = yearly[:, :LANES]
        kept[group, me_year] = yearly[:, LANES:]
        for step in range(1, n_year):
            copy = year_copy(step, group)
            copy.start()
            copies.append(copy)
        reinstated = reinst_ref[:, lanes].astype(jnp.float32)
        layer_paid = jnp.minimum(annual, (1.0 + reinstated) * limit_loss)
        net_ref[:, lanes] = (
            layer_paid
            - rate_ref[:, lanes] * jnp.minimum(layer_paid, reinstated * limit_loss)
        ) / limit_loss

    for group in range(groups):
        lanes = slice(group * LANES, (group + 1) * LANES)
        for step in range(1, n_year):
            source = lax.rem(me_year + step, n_year)
            pltpu.make_async_remote_copy(
                src_ref=kept.at[group, source],
                dst_ref=kept.at[group, source],
                send_sem=year_send.at[group, step - 1],
                recv_sem=year_recv.at[group, source],
                device_id={"year": source},
                device_id_type=MESH,
            ).wait_recv()
        every = kept[group].reshape(n_year * YEAR_DEV, LANES)
        base_loss = UNIT_LOSS + jnp.sum(every, axis=0, keepdims=True) / (n_year * YEAR_DEV)
        tail_ref[:, lanes] = largest_sum(every) / base_loss / TAIL
        loss_ratio = kept[group, me_year] / base_loss
        stop_ref[:, lanes] = clamp_between(
            loss_ratio - stop_attach_ref[:, lanes], 0.0, stop_width_ref[:, lanes]
        )

    for copy in copies:
        copy.wait_send()


def put_out(*refs):
    results, outputs, sem = refs[:3], refs[3:6], refs[6]
    moves = [
        pltpu.make_async_copy(result, output, sem.at[index])
        for index, (result, output) in enumerate(zip(results, outputs))
    ]
    for move in moves:
        move.start()
    for move in moves:
        move.wait()


def on_device(sizes, event_loss, event_year, retention, risk_limit, share, member, *terms):
    n_year, n_port, own, groups = sizes
    rows, ports = event_loss.shape
    padded = groups * LANES

    def row(values):
        return values.reshape(1, values.shape[0])

    def term_row(values):
        if padded != own:
            values = jnp.pad(values, (0, padded - own), constant_values=1)
        return row(values)

    operands = [
        event_loss,
        row(event_year),
        row(retention),
        row(risk_limit),
        share.T,
        member.T,
        *[term_row(values) for values in terms],
    ]
    anywhere = pl.BlockSpec(memory_space=pl.ANY)
    vmem = pl.BlockSpec(memory_space=pltpu.VMEM)
    pieces = n_port - 1
    shapes = [(YEAR_DEV, padded), (YEAR_DEV, padded), (1, padded)]
    results = pl.pallas_call(
        functools.partial(kernel, sizes),
        name="layers",
        out_shape=[pltpu.VMEM(shape, jnp.float32) for shape in shapes],
        in_specs=[anywhere] * len(operands),
        out_specs=[vmem] * len(shapes),
        scratch_shapes=[
            *[pltpu.VMEM(operand.shape, operand.dtype) for operand in operands],
            pltpu.VMEM((LANES, ports), jnp.bfloat16),
            pltpu.VMEM((rows, ports), jnp.bfloat16),
            pltpu.VMEM((pieces, groups, rows, LANES), jnp.bfloat16),
            pltpu.VMEM((pieces, groups, rows, LANES), jnp.bfloat16),
            pltpu.VMEM((groups, rows, LANES), jnp.float32),
            pltpu.VMEM((groups, rows, LANES), jnp.float32),
            pltpu.VMEM((groups, n_year, YEAR_DEV, LANES), jnp.float32),
            pltpu.SemaphoreType.DMA((CHUNKS,)),
            pltpu.SemaphoreType.DMA((len(operands),)),
            pltpu.SemaphoreType.DMA((pieces, groups, CHUNKS)),
            pltpu.SemaphoreType.DMA((pieces, groups, CHUNKS)),
            pltpu.SemaphoreType.DMA((groups, n_year)),
            pltpu.SemaphoreType.DMA((groups, n_year)),
        ],
        compiler_params=pltpu.CompilerParams(collective_id=0, has_side_effects=True),
    )(*operands)
    layer_net, stop_loss, tail_mean = pl.pallas_call(
        put_out,
        name="put_out",
        out_shape=[jax.ShapeDtypeStruct(shape, jnp.float32) for shape in shapes],
        in_specs=[anywhere] * len(shapes),
        out_specs=[anywhere] * len(shapes),
        scratch_shapes=[pltpu.SemaphoreType.DMA((len(shapes),))],
    )(*[pltpu.with_memory_space_constraint(value, pltpu.VMEM) for value in results])
    return layer_net[:, :own].T, stop_loss[:, :own].T, tail_mean[0, :own]


def solution(mesh):
    n_year, n_port = mesh.shape["year"], mesh.shape["port"]
    own = TREATIES // n_port
    groups = -(-own // LANES)
    return jax.shard_map(
        functools.partial(on_device, (n_year, n_port, own, groups)),
        mesh=mesh,
        in_specs=(
            P("year", "port"),
            P("year"),
            P("port"),
            P("port"),
            P("port", None),
            P("port", None),
            P("port"),
            P("port"),
            P("port"),
            P("port"),
            P("port"),
            P("port"),
        ),
        out_specs=(P("port", "year"), P("port", "year"), P("port")),
        check_vma=False,
    )
```
